32 devices in a mesh: groups: 2 (over y), wide: 4 (over x, core), tp: 4 (over z).
Axes of the slice: x: 2, y: 2, z: 4, core: 2. Of those that a mesh axis runs over, the one named last changes fastest.
Arguments:
- patches: bfloat16 [2048, 1280], P(('groups', 'wide')), parts along dimension 0, may hold values from -190 to 190
- patch_counts: int32 [64], P('groups'), parts along dimension 0, may hold values from 24 to 32, as said below
- placement: int32 [64, 2], P('groups'), parts along dimension 0, may hold values from 0 to 511, as said below
- positions: int32 [3, 4096], P(None, ('groups', 'wide')), parts along dimension 1, may hold values from 0 to 2047
- text_embeds: bfloat16 [4096, 8192], P(('groups', 'wide'), 'tp'), parts along dimension 0, may hold values from -180 to 180
- vit_gain: float32 [1280], replicated, may hold values from 0.1 to 1.9
- vit_qkv: bfloat16 [1280, 3, 1280], P(None, None, 'tp'), may hold values from -4 to 4
- vit_proj: bfloat16 [1280, 1280], P('tp'), may hold values from -0.15625 to 0.15625
- merger_gain: float32 [1280], replicated, may hold values from 0.1 to 1.9
- merger_up: bfloat16 [5120, 2560], P(None, 'tp'), may hold values from -0.078125 to 0.078125
- merger_down: bfloat16 [2560, 8192], P('tp'), may hold values from -0.15625 to 0.15625
- llm_gain: float32 [8192], replicated, may hold values from 0.1 to 1.9
- llm_query: bfloat16 [8192, 4096], P('wide', 'tp'), may hold values from -0.0625 to 0.0625
- llm_key: bfloat16 [8192, 1024], P('wide', 'tp'), may hold values from -0.0625 to 0.0625
- llm_value: bfloat16 [8192, 1024], P('wide', 'tp'), may hold values from -0.0625 to 0.0625
Outputs:
- query: bfloat16 [4096, 4096], P(('groups', 'wide'), 'tp'), parts along dimension 0
- key_cache: bfloat16 [4096, 1024], P(('groups', 'wide'), 'tp'), parts along dimension 0
- value_cache: bfloat16 [4096, 1024], P(('groups', 'wide'), 'tp'), parts along dimension 0
The draws below stay inside these ranges and needn't reach their ends.
There are 2 independent parts, one for each index of `groups`. The reference program is written for one: setup_inputs(seed, part) draws one part's arguments, and reference() takes and returns one part's arrays. A program takes and returns all parts, laid end to end along the dimension named above; an argument that names none is the same for every part. Nothing has to cross between parts.
Inputs may be any that keep to these rules, and one draw needn't show every extreme that they name: `patch_counts`: each count is a multiple of 4; images 8 * s to 8 * s + 7 belong to encoder device s of the wide axis; patch rows 4 m to 4 m + 3 of an image form its merged row m. `placement`: column 0 is the owner on the wide axis, column 1 the first of the image's merged rows among that owner's 512 rows. Images' merged rows never intersect and stay within the owner's rows. Each owner receives 8 images. At most 16 merged rows go from one encoder device to one owner, and that number is reached in every draw.
All inputs are finite; a program needn't handle non-finite values.
Results may differ from the reference program's by a relative error of at most 0.015.
Values may be sent and summed in bfloat16 or wider, within the bound.
A program may use at most 128 MiB of HBM per device.

```python
import jax
import jax.numpy as jnp
from jax import lax

VD = 1280
VH = 16
LD = 8192
KVH = 8
HD = 128
QH = 32
MH = 2560
IMG_DEV = 8
MAXP = 32
TOK_DEV = 512
VHD = 80
MAXM = 8
IMAGES = 32
TOKENS = 2048
N_TP = 4


def layout_tables(key):
    width_wide = IMAGES // IMG_DEV
    rank_key, owner_key, count_key, shift_key = jax.random.split(jax.random.fold_in(key, 7), 4)
    source_rank = jax.random.permutation(rank_key, width_wide).astype(jnp.int32)
    owner_order = jax.random.permutation(owner_key, width_wide).astype(jnp.int32)
    image_ids = jnp.arange(IMAGES, dtype=jnp.int32)
    source = image_ids // IMG_DEV
    within = image_ids % IMG_DEV
    owner_ids = owner_order[(source_rank[source] + within) % width_wide]
    lowest = max(1, 3 * MAXM // 4)
    merged = jax.random.randint(count_key, (IMAGES,), lowest, MAXM + 1).astype(jnp.int32)
    forced = (source == 0) & (within % width_wide == 0)
    merged = jnp.where(forced, MAXM, merged).astype(jnp.int32)
    slot_rows = TOK_DEV // IMG_DEV
    shift_rows = jax.random.randint(shift_key, (IMAGES,), 0, slot_rows - merged + 1).astype(jnp.int32)
    start_rows = within * slot_rows + shift_rows
    return (merged * 4, jnp.stack([owner_ids, start_rows], axis=1))


def draw_patch_counts(key, part):
    return layout_tables(key)[0].astype(jnp.int32)


def draw_placement(key, part):
    return layout_tables(key)[1].astype(jnp.int32)


def draw_patches(key, part):
    base_key = jax.random.fold_in(jax.random.fold_in(key, 13), 0)
    total_rows = IMAGES * MAXP
    field = jnp.clip(jax.random.normal(base_key, (total_rows, VD), jnp.float32), -4.0, 4.0)
    return field.astype(jnp.bfloat16)


def draw_text_embeds(key, part):
    base_key = jax.random.fold_in(jax.random.fold_in(key, 17), 0)
    field = jnp.clip(jax.random.normal(base_key, (TOKENS, LD), jnp.float32), -4.0, 4.0)
    return field.astype(jnp.bfloat16)


def draw_vit_qkv(key, part):
    base_key = jax.random.fold_in(jax.random.fold_in(key, 11), 0)
    base = jnp.clip(jax.random.normal(base_key, (VD, 3, VD), jnp.float32), -4.0, 4.0) * VD ** (-0.5)
    return base.astype(jnp.bfloat16)


def plant(drawn, rng, low, top_value):
    place = [jax.random.randint(jax.random.fold_in(rng, axis), (), 0, length) for axis, length in enumerate(drawn.shape)]
    widest = drawn.shape.index(max(drawn.shape))
    beside = place[:widest] + [(place[widest] + 1) % drawn.shape[widest]] + place[widest + 1:]
    return drawn.at[tuple(place)].set(low).at[tuple(beside)].set(top_value)


def spiked(result, rng, source, target, parts, factor):
    owner, partner = [(jnp.arange(result.shape[dim]) // (result.shape[dim] // parts)).reshape([-1 if axis == dim else 1 for axis in range(result.ndim)]) for dim in (source, target)]
    chosen = jax.random.permutation(rng, parts)[partner]
    strong = (owner == chosen) | (owner == (partner + parts // 2) % parts)
    return jnp.where(strong, factor * result, result)


def block_levels(stream_key, extent, shards, least, high):
    def one(dim, blocks):
        draws = jax.random.uniform(jax.random.fold_in(jax.random.fold_in(stream_key, 6), dim), (blocks,), jnp.float32, least / len(shards), high / len(shards))
        return jnp.repeat(jnp.exp(draws), extent[dim] // blocks).reshape((-1,) + (1,) * (len(extent) - dim - 1))

    gain = one(*shards[0])
    for cut in shards[1:]:
        gain = gain * one(*cut)
    return gain


def bell_draw(key, extent, scale, most, cuts=(), kind=jnp.bfloat16):
    drawn = scale * jax.random.normal(key, extent, jnp.float32)
    if cuts:
        drawn = drawn * block_levels(key, extent, cuts, -0.22, 0.18)
    return jnp.clip(drawn, -most, most).astype(kind)


def heavy_noise(own_key, dims, scale, bound, shards, heavy, kind=jnp.bfloat16):
    array = scale * jax.random.normal(own_key, dims, jnp.float32)
    if shards:
        array = array * block_levels(own_key, dims, shards, -0.22, 0.18)
    return jnp.clip(spiked(array, jax.random.fold_in(own_key, 3), *heavy), -bound, bound).astype(kind)


def setup_inputs(seed: int = 0, part: int = 0) -> dict:
    keys = jax.random.split(jax.random.key(seed), 16)
    part_splits = jax.random.split(jax.random.fold_in(keys[15], part), 16)
    return {
        "patches": draw_patches(jax.random.fold_in(jax.random.fold_in(keys[15], part), 71), part),
        "patch_counts": draw_patch_counts(jax.random.fold_in(jax.random.fold_in(keys[15], part), 71), part),
        "placement": draw_placement(jax.random.fold_in(jax.random.fold_in(keys[15], part), 71), part),
        "positions": plant(jax.random.randint(part_splits[3], (3, TOKENS), 0, TOKENS), jax.random.fold_in(part_splits[3], 1), 0, TOKENS - 1).astype(jnp.int32),
        "text_embeds": draw_text_embeds(jax.random.fold_in(jax.random.fold_in(keys[15], part), 71), part),
        "vit_gain": jnp.clip(1.0 + 0.18 * jax.random.normal(keys[5], (VD,), jnp.float32), 0.1, 1.9),
        "vit_qkv": draw_vit_qkv(jax.random.fold_in(keys[15], 71), part),
        "vit_proj": bell_draw(keys[7], (VD, VD), VD ** -0.5, 0.15625, ((0, 4),)),
        "merger_gain": jnp.clip(1.0 + 0.18 * jax.random.normal(keys[8], (VD,), jnp.float32), 0.1, 1.9),
        "merger_up": bell_draw(keys[9], (4 * VD, MH), (4 * VD) ** -0.5, 0.078125, ((1, 4),)),
        "merger_down": heavy_noise(keys[10], (MH, LD), MH ** -0.5, 0.15625, ((0, 4),), (0, 1, 4, 2.0)),
        "llm_gain": jnp.clip(1.0 + 0.18 * jax.random.normal(keys[11], (LD,), jnp.float32), 0.1, 1.9),
        "llm_query": bell_draw(keys[12], (LD, QH * HD), LD ** -0.5, 0.0625, ((0, 4), (1, 4))),
        "llm_key": bell_draw(keys[13], (LD, KVH * HD), LD ** -0.5, 0.0625, ((0, 4), (1, 4))),
        "llm_value": bell_draw(keys[14], (LD, KVH * HD), LD ** -0.5, 0.0625, ((0, 4), (1, 4))),
    }


NORM_EPS = 1e-06
ROPE_BASE = 1000000.0

def layer_norm(inputs, scale_gain):
    center = lax.optimization_barrier(jnp.mean(inputs, axis=-1, keepdims=True))
    shifted = inputs - center
    spread = lax.optimization_barrier(jnp.mean(shifted * shifted, axis=-1, keepdims=True))
    return shifted * lax.rsqrt(spread + NORM_EPS) * scale_gain

def rms_norm(inputs, scale_gain):
    square = lax.optimization_barrier(jnp.mean(inputs * inputs, axis=-1, keepdims=True))
    return inputs * lax.rsqrt(square + NORM_EPS) * scale_gain

def rotary(values, positions):
    half_size = HD // 2
    frequency = jnp.arange(half_size).astype(jnp.float32)
    inverse = ROPE_BASE ** (-2.0 * frequency / HD)
    first_end = HD // 8
    second = first_end + 3 * HD // 16
    ordinal = jnp.arange(half_size)
    section = jnp.where(ordinal < first_end, 0, jnp.where(ordinal < second, 1, 2))
    chosen = jnp.where(section[:, None] == 0, positions[0][None, :], jnp.where(section[:, None] == 1, positions[1][None, :], positions[2][None, :]))
    angles = chosen.T.astype(jnp.float32) * inverse[None, :]
    angles = jnp.concatenate([angles, angles], axis=1)
    cosine = jnp.cos(angles)[:, None, :]
    sine_table = jnp.sin(angles)[:, None, :]
    upper_half = values[..., :half_size]
    lower_half = values[..., half_size:]
    turned = jnp.concatenate([-lower_half, upper_half], axis=-1)
    return values * cosine + turned * sine_table

def reference(patches, patch_counts, placement, positions, text_embeds, vit_gain, vit_qkv, vit_proj, merger_gain, merger_up, merger_down, llm_gain, llm_query, llm_key, llm_value):
    patch_rows = patches.astype(jnp.float32)
    normed = layer_norm(patch_rows, vit_gain).astype(jnp.bfloat16)
    triple = jnp.dot(normed, vit_qkv.reshape(VD, 3 * VD), preferred_element_type=jnp.float32)
    triple = lax.optimization_barrier(triple.astype(jnp.bfloat16))
    triple = triple.reshape(IMAGES, MAXP, 3, VH, VHD).astype(jnp.float32)
    scores = jnp.einsum('iqhd,ikhd->ihqk', triple[:, :, 0], triple[:, :, 1]) * VHD ** (-0.5)
    present = jnp.arange(MAXP)[None, :] < patch_counts[:, None]
    scores = jnp.where(present[:, None, None, :], scores, -jnp.inf)
    highest = lax.optimization_barrier(jnp.max(scores, axis=-1, keepdims=True))
    raised = jnp.exp(scores - highest)
    attention_weights = (raised / lax.optimization_barrier(jnp.sum(raised, axis=-1, keepdims=True))).astype(jnp.bfloat16)
    attention_weights = lax.optimization_barrier(attention_weights).astype(jnp.float32)
    context = jnp.einsum('ihqk,ikhd->iqhd', attention_weights, triple[:, :, 2])
    context = context.astype(jnp.bfloat16).reshape(IMAGES * MAXP, VD)
    group_width = VD // N_TP
    attended = jnp.zeros((IMAGES * MAXP, VD), jnp.float32)
    for member in range(N_TP):
        share = jnp.dot(context[:, member * group_width:(member + 1) * group_width], vit_proj[member * group_width:(member + 1) * group_width], preferred_element_type=jnp.float32)
        attended = attended + lax.optimization_barrier(share.astype(jnp.bfloat16)).astype(jnp.float32)
    mixed_rows = patch_rows + attended
    merged_in = layer_norm(mixed_rows, merger_gain).astype(jnp.bfloat16).reshape(IMAGES * MAXM, 4 * VD)
    hidden = jax.nn.gelu(jnp.dot(merged_in, merger_up, preferred_element_type=jnp.float32), approximate=False).astype(jnp.bfloat16)
    unit_width = MH // N_TP
    summed = jnp.zeros((IMAGES * MAXM, LD), jnp.float32)
    for member in range(N_TP):
        share = jnp.dot(hidden[:, member * unit_width:(member + 1) * unit_width], merger_down[member * unit_width:(member + 1) * unit_width], preferred_element_type=jnp.float32)
        summed = summed + lax.optimization_barrier(share.astype(jnp.bfloat16)).astype(jnp.float32)
    visual = summed.astype(jnp.bfloat16)
    merged_count = patch_counts // 4
    offsets = jnp.arange(MAXM).astype(jnp.int32)
    targets = placement[:, 0:1] * TOK_DEV + placement[:, 1:2] + offsets[None, :]
    targets = jnp.where(offsets[None, :] < merged_count[:, None], targets, TOKENS).astype(jnp.int32)
    prompt_rows = text_embeds.at[targets.reshape(-1)].set(visual, mode='drop')
    normed_prompt = rms_norm(prompt_rows.astype(jnp.float32), llm_gain).astype(jnp.bfloat16)
    queries = jnp.dot(normed_prompt, llm_query, preferred_element_type=jnp.float32).reshape(TOKENS, QH, HD)
    queries = rotary(queries, positions).astype(jnp.bfloat16).reshape(TOKENS, QH * HD)
    key_rows = jnp.dot(normed_prompt, llm_key, preferred_element_type=jnp.float32).reshape(TOKENS, KVH, HD)
    key_rows = rotary(key_rows, positions).astype(jnp.bfloat16).reshape(TOKENS, KVH * HD)
    value_rows = jnp.dot(normed_prompt, llm_value, preferred_element_type=jnp.float32).astype(jnp.bfloat16)
    return (queries, key_rows, value_rows)
```

```python
import jax
import jax.numpy as jnp
from jax import lax
from jax.sharding import PartitionSpec as P

VD = 1280
HD = 128
IMG_DEV = 8
MAXP = 32
TOK_DEV = 512
VHD = 80
MAXM = 8


NORM_EPS = 1e-06
ROPE_BASE = 1000000.0


def layer_norm(inputs, scale_gain):
    center = jnp.mean(inputs, axis=-1, keepdims=True)
    shifted = inputs - center
    spread = jnp.mean(shifted * shifted, axis=-1, keepdims=True)
    return shifted * lax.rsqrt(spread + NORM_EPS) * scale_gain


def rms_norm(inputs, scale_gain):
    square = jnp.mean(inputs * inputs, axis=-1, keepdims=True)
    return inputs * lax.rsqrt(square + NORM_EPS) * scale_gain


def rotary(values, positions):
    half_size = HD // 2
    frequency = jnp.arange(half_size).astype(jnp.float32)
    inverse = ROPE_BASE ** (-2.0 * frequency / HD)
    first_end = HD // 8
    second = first_end + 3 * HD // 16
    ordinal = jnp.arange(half_size)
    section = jnp.where(ordinal < first_end, 0, jnp.where(ordinal < second, 1, 2))
    chosen = jnp.where(
        section[:, None] == 0,
        positions[0][None, :],
        jnp.where(section[:, None] == 1, positions[1][None, :], positions[2][None, :]),
    )
    angles = chosen.T.astype(jnp.float32) * inverse[None, :]
    angles = jnp.concatenate([angles, angles], axis=1)
    cosine = jnp.cos(angles)[:, None, :]
    sine_table = jnp.sin(angles)[:, None, :]
    upper_half = values[..., :half_size]
    lower_half = values[..., half_size:]
    turned = jnp.concatenate([-lower_half, upper_half], axis=-1)
    return values * cosine + turned * sine_table


def handoff_tables(patch_counts, placement, width_wide, myself, capacity):
    merged_count = patch_counts // 4
    owners = placement[:, 0]
    starts = placement[:, 1]
    owner_grid = owners.reshape(width_wide, IMG_DEV)
    count_grid = merged_count.reshape(width_wide, IMG_DEV)
    ordinal = jnp.arange(IMG_DEV)
    before = ordinal[:, None] < ordinal[None, :]
    same_owner = owner_grid[:, :, None] == owner_grid[:, None, :]
    offsets = jnp.sum(jnp.where(same_owner & before[None], count_grid[:, :, None], 0), axis=1)
    mine_owner = lax.dynamic_index_in_dim(owner_grid, myself, 0, keepdims=False)
    mine_count = lax.dynamic_index_in_dim(count_grid, myself, 0, keepdims=False)
    mine_offset = lax.dynamic_index_in_dim(offsets, myself, 0, keepdims=False)
    target = jnp.arange(width_wide)[:, None, None]
    slot_index = jnp.arange(capacity)[None, :, None]
    matches = (
        (mine_owner[None, None, :] == target)
        & (slot_index >= mine_offset[None, None, :])
        & (slot_index < mine_offset[None, None, :] + mine_count[None, None, :])
    )
    source_row = ordinal[None, None, :] * MAXM + slot_index - mine_offset[None, None, :]
    send_index = jnp.sum(jnp.where(matches, source_row, 0), axis=-1)
    send_live = jnp.any(matches, axis=-1)
    row_place = jnp.arange(TOK_DEV)[:, None]
    inside = (
        (owners[None, :] == myself)
        & (row_place >= starts[None, :])
        & (row_place < starts[None, :] + merged_count[None, :])
    )
    image_source = jnp.arange(owners.shape[0]) // IMG_DEV
    flat_slot = (
        image_source[None, :] * capacity
        + offsets.reshape(-1)[None, :]
        + row_place
        - starts[None, :]
    )
    take_index = jnp.sum(jnp.where(inside, flat_slot, 0), axis=-1)
    take_live = jnp.any(inside, axis=-1)
    return (send_index, send_live, take_index, take_live)


def pack_rows(visual, send_index, send_live):
    picked = jnp.take(visual, send_index.reshape(-1), axis=0)
    picked = picked.reshape(send_index.shape + (visual.shape[1],))
    return jnp.where(send_live[..., None], picked, jnp.zeros((), visual.dtype))


def exchange_sum(partial, axis_name, split_axis):
    members = lax.axis_size(axis_name)
    shape = partial.shape
    cut = shape[:split_axis] + (members, shape[split_axis] // members) + shape[split_axis + 1 :]
    stacked = jnp.moveaxis(partial.reshape(cut), split_axis, 0)
    swapped = lax.all_to_all(stacked, axis_name, split_axis=0, concat_axis=0, tiled=True)
    return jnp.sum(swapped.astype(jnp.float32), axis=0)


def doubling_gather(block, axis_name):
    members = lax.axis_size(axis_name)
    held = {0: block}
    bits = []
    step = 1
    while step < members:
        bits.append(step)
        step *= 2
    for bit in bits[1:] + bits[:1]:
        pairs = [(source, source ^ bit) for source in range(members)]
        for entry in sorted(held):
            held[entry ^ bit] = lax.ppermute(held[entry], axis_name, pairs)
    return [held[entry] for entry in range(members)]


def ring_gather_columns(block, axis_name):
    members = lax.axis_size(axis_name)
    me = lax.axis_index(axis_name)
    width = block.shape[1]
    up = [(source, (source + 1) % members) for source in range(members)]
    down = [(source, (source - 1) % members) for source in range(members)]
    gathered = jnp.zeros((block.shape[0], width * members), block.dtype)
    pieces = [(0, 0, block)]
    forward, backward = block, block
    distance = 1
    while 2 * distance < members:
        forward = lax.ppermute(forward, axis_name, up)
        backward = lax.ppermute(backward, axis_name, down)
        pieces.append((members - distance, 0, forward))
        pieces.append((distance, 0, backward))
        distance += 1
    if 2 * distance == members:
        half = width // 2
        pieces.append((distance, 0, lax.ppermute(forward[:, :half], axis_name, up)))
        pieces.append((distance, half, lax.ppermute(backward[:, half:], axis_name, down)))
    for offset, inner, piece in pieces:
        column = lax.rem(me + offset, members) * width + inner
        gathered = lax.dynamic_update_slice(gathered, piece, (0, column))
    return gathered


def project(rows, weight_blocks, member):
    depth = weight_blocks[0].shape[0]
    total = None
    for entry, block in enumerate(weight_blocks):
        columns = lax.dynamic_slice_in_dim(rows, (member ^ entry) * depth, depth, 1)
        share = jnp.dot(columns, block, preferred_element_type=jnp.float32)
        total = share if total is None else total + share
    return total


def per_device(
    patches,
    patch_counts,
    placement,
    positions,
    text_embeds,
    vit_gain,
    vit_qkv,
    vit_proj,
    merger_gain,
    merger_up,
    merger_down,
    llm_gain,
    llm_query,
    llm_key,
    llm_value,
):
    width_wide = lax.axis_size("wide")
    myself = lax.axis_index("wide")
    capacity = MAXM * ((IMG_DEV + width_wide - 1) // width_wide)
    local_heads = vit_qkv.shape[2] // VHD
    own_weights = jnp.concatenate([llm_query, llm_key, llm_value], axis=1)
    weight_blocks = doubling_gather(own_weights, "wide")
    text_rows = ring_gather_columns(text_embeds, "tp")
    members = lax.axis_size("tp")
    patch_rows = patches.astype(jnp.float32)
    normed = layer_norm(patch_rows, vit_gain).astype(jnp.bfloat16)
    triple = jnp.dot(normed, vit_qkv.reshape(VD, -1), preferred_element_type=jnp.float32).astype(
        jnp.bfloat16
    )
    triple = triple.reshape(IMG_DEV, MAXP, 3, local_heads, VHD)
    scores = jnp.einsum(
        "iqhd,ikhd->ihqk", triple[:, :, 0], triple[:, :, 1], preferred_element_type=jnp.float32
    ) * VHD ** (-0.5)
    own_counts = lax.dynamic_slice_in_dim(patch_counts, myself * IMG_DEV, IMG_DEV)
    present = jnp.arange(MAXP)[None, :] < own_counts[:, None]
    scores = jnp.where(present[:, None, None, :], scores, -jnp.inf)
    highest = jnp.max(scores, axis=-1, keepdims=True)
    raised = jnp.exp(scores - highest)
    attention_weights = (raised / jnp.sum(raised, axis=-1, keepdims=True)).astype(jnp.bfloat16)
    context = jnp.einsum(
        "ihqk,ikhd->iqhd", attention_weights, triple[:, :, 2], preferred_element_type=jnp.float32
    ).astype(jnp.bfloat16)
    context = context.reshape(IMG_DEV * MAXP, local_heads * VHD)
    partial_heads = jnp.dot(context, vit_proj, preferred_element_type=jnp.float32)
    attended = exchange_sum(partial_heads.astype(jnp.bfloat16), "tp", 0)
    own_rows = IMG_DEV * MAXP // members
    own_patches = lax.dynamic_slice_in_dim(patches, lax.axis_index("tp") * own_rows, own_rows, 0)
    mixed_rows = own_patches.astype(jnp.float32) + attended
    own_merged = layer_norm(mixed_rows, merger_gain).astype(jnp.bfloat16)
    own_merged = own_merged.reshape(own_rows * MAXM // MAXP, 4 * VD)
    merged_in = lax.all_gather(own_merged, "tp", axis=0, tiled=True)
    hidden = jax.nn.gelu(
        jnp.dot(merged_in, merger_up, preferred_element_type=jnp.float32), approximate=False
    ).astype(jnp.bfloat16)
    partial_visual = jnp.dot(hidden, merger_down, preferred_element_type=jnp.float32)
    send_index, send_live, take_index, take_live = handoff_tables(
        patch_counts, placement, width_wide, myself, capacity
    )
    visual = exchange_sum(partial_visual.astype(jnp.bfloat16), "tp", 1).astype(jnp.bfloat16)
    outgoing = pack_rows(visual, send_index, send_live)
    incoming = lax.all_to_all(outgoing, "wide", split_axis=0, concat_axis=0, tiled=True)
    incoming = incoming.reshape(-1, incoming.shape[-1])
    copies = jnp.broadcast_to(incoming[None], (members,) + incoming.shape)
    spread_rows = lax.all_to_all(copies, "tp", split_axis=0, concat_axis=0, tiled=True)
    visual_rows = jnp.swapaxes(spread_rows, 0, 1).reshape(incoming.shape[0], -1)
    normed_text = rms_norm(text_rows.astype(jnp.float32), llm_gain).astype(jnp.bfloat16)
    normed_visual = rms_norm(visual_rows.astype(jnp.float32), llm_gain).astype(jnp.bfloat16)
    projected_text = project(normed_text, weight_blocks, myself)
    projected_visual = project(normed_visual, weight_blocks, myself)
    placed = jnp.take(projected_visual, take_index, axis=0)
    projected = jnp.where(take_live[:, None], placed, projected_text)
    first = llm_query.shape[1]
    second = first + llm_key.shape[1]
    projected_query = projected[:, :first]
    projected_key = projected[:, first:second]
    projected_value = projected[:, second:]
    queries = (
        rotary(projected_query.reshape(TOK_DEV, -1, HD), positions)
        .astype(jnp.bfloat16)
        .reshape(TOK_DEV, -1)
    )
    key_rows = (
        rotary(projected_key.reshape(TOK_DEV, -1, HD), positions)
        .astype(jnp.bfloat16)
        .reshape(TOK_DEV, -1)
    )
    value_rows = projected_value.astype(jnp.bfloat16)
    return (queries, key_rows, value_rows)


def solution(mesh):
    return jax.shard_map(
        per_device,
        mesh=mesh,
        in_specs=(
            P(("groups", "wide"), None),
            P("groups"),
            P("groups", None),
            P(None, ("groups", "wide")),
            P(("groups", "wide"), "tp"),
            P(),
            P(None, None, "tp"),
            P("tp", None),
            P(),
            P(None, "tp"),
            P("tp", None),
            P(),
            P("wide", "tp"),
            P("wide", "tp"),
            P("wide", "tp"),
        ),
        out_specs=(
            P(("groups", "wide"), "tp"),
            P(("groups", "wide"), "tp"),
            P(("groups", "wide"), "tp"),
        ),
        check_vma=False,
    )
```

```python
import jax
import jax.numpy as jnp
from jax import lax
from jax.sharding import PartitionSpec as P

VD = 1280
HD = 128
IMG_DEV = 8
MAXP = 32
TOK_DEV = 512
VHD = 80
MAXM = 8


NORM_EPS = 1e-06
ROPE_BASE = 1000000.0


def layer_norm(inputs, scale_gain):
    center = jnp.mean(inputs, axis=-1, keepdims=True)
    shifted = inputs - center
    spread = jnp.mean(shifted * shifted, axis=-1, keepdims=True)
    return shifted * lax.rsqrt(spread + NORM_EPS) * scale_gain


def rms_norm(inputs, scale_gain):
    square = jnp.mean(inputs * inputs, axis=-1, keepdims=True)
    return inputs * lax.rsqrt(square + NORM_EPS) * scale_gain


def rotary_tables(positions):
    half_size = HD // 2
    frequency = jnp.arange(half_size).astype(jnp.float32)
    inverse = ROPE_BASE ** (-2.0 * frequency / HD)
    first_end = HD // 8
    second = first_end + 3 * HD // 16
    ordinal = jnp.arange(half_size)
    section = jnp.where(ordinal < first_end, 0, jnp.where(ordinal < second, 1, 2))
    chosen = jnp.where(
        section[:, None] == 0,
        positions[0][None, :],
        jnp.where(section[:, None] == 1, positions[1][None, :], positions[2][None, :]),
    )
    angles = chosen.T.astype(jnp.float32) * inverse[None, :]
    angles = jnp.concatenate([angles, angles], axis=1)
    cosine = jnp.cos(angles)[:, None, :]
    sine_table = jnp.sin(angles)[:, None, :]
    return cosine, sine_table


def rotary(values, tables):
    cosine, sine_table = tables
    half_size = HD // 2
    upper_half = values[..., :half_size]
    lower_half = values[..., half_size:]
    turned = jnp.concatenate([-lower_half, upper_half], axis=-1)
    return values * cosine + turned * sine_table


def handoff_tables(patch_counts, placement, width_wide, myself, capacity):
    merged_count = patch_counts // 4
    owners = placement[:, 0]
    starts = placement[:, 1]
    owner_grid = owners.reshape(width_wide, IMG_DEV)
    count_grid = merged_count.reshape(width_wide, IMG_DEV)
    ordinal = jnp.arange(IMG_DEV)
    before = ordinal[:, None] < ordinal[None, :]
    same_owner = owner_grid[:, :, None] == owner_grid[:, None, :]
    offsets = jnp.sum(jnp.where(same_owner & before[None], count_grid[:, :, None], 0), axis=1)
    mine_owner = lax.dynamic_index_in_dim(owner_grid, myself, 0, keepdims=False)
    mine_count = lax.dynamic_index_in_dim(count_grid, myself, 0, keepdims=False)
    mine_offset = lax.dynamic_index_in_dim(offsets, myself, 0, keepdims=False)
    target = jnp.arange(width_wide)[:, None, None]
    slot_index = jnp.arange(capacity)[None, :, None]
    matches = (
        (mine_owner[None, None, :] == target)
        & (slot_index >= mine_offset[None, None, :])
        & (slot_index < mine_offset[None, None, :] + mine_count[None, None, :])
    )
    source_row = ordinal[None, None, :] * MAXM + slot_index - mine_offset[None, None, :]
    send_index = jnp.sum(jnp.where(matches, source_row, 0), axis=-1)
    send_live = jnp.any(matches, axis=-1)
    row_place = jnp.arange(TOK_DEV)[:, None]
    inside = (
        (owners[None, :] == myself)
        & (row_place >= starts[None, :])
        & (row_place < starts[None, :] + merged_count[None, :])
    )
    image_source = jnp.arange(owners.shape[0]) // IMG_DEV
    flat_slot = (
        image_source[None, :] * capacity
        + offsets.reshape(-1)[None, :]
        + row_place
        - starts[None, :]
    )
    take_index = jnp.sum(jnp.where(inside, flat_slot, 0), axis=-1)
    take_live = jnp.any(inside, axis=-1)
    return (send_index, send_live, take_index, take_live)


def place_rows(incoming, take_index, take_live, text_rows):
    picked = jnp.take(incoming, take_index, axis=0)
    return jnp.where(take_live[:, None], picked, text_rows)


def pack_rows(visual, send_index, send_live):
    picked = jnp.take(visual, send_index.reshape(-1), axis=0)
    picked = picked.reshape(send_index.shape + (visual.shape[1],))
    return jnp.where(send_live[..., None], picked, jnp.zeros((), visual.dtype))


def exchange_sum(partial, axis_name, split_axis):
    members = lax.axis_size(axis_name)
    shape = partial.shape
    cut = shape[:split_axis] + (members, shape[split_axis] // members) + shape[split_axis + 1 :]
    stacked = jnp.moveaxis(partial.reshape(cut), split_axis, 0)
    swapped = lax.all_to_all(stacked, axis_name, split_axis=0, concat_axis=0, tiled=True)
    return jnp.sum(swapped.astype(jnp.float32), axis=0)


def doubling_gather(block, axis_name):
    members = lax.axis_size(axis_name)
    held = {0: block}
    bits = []
    step = 1
    while step < members:
        bits.append(step)
        step *= 2
    for bit in bits[1:] + bits[:1]:
        pairs = [(source, source ^ bit) for source in range(members)]
        for entry in sorted(held):
            held[entry ^ bit] = lax.ppermute(held[entry], axis_name, pairs)
    return [held[entry] for entry in range(members)]


def ring_gather_columns(block, axis_name):
    members = lax.axis_size(axis_name)
    me = lax.axis_index(axis_name)
    width = block.shape[1]
    up = [(source, (source + 1) % members) for source in range(members)]
    down = [(source, (source - 1) % members) for source in range(members)]
    gathered = jnp.zeros((block.shape[0], width * members), block.dtype)
    pieces = [(0, 0, block)]
    forward, backward = block, block
    distance = 1
    while 2 * distance < members:
        forward = lax.ppermute(forward, axis_name, up)
        backward = lax.ppermute(backward, axis_name, down)
        pieces.append((members - distance, 0, forward))
        pieces.append((distance, 0, backward))
        distance += 1
    if 2 * distance == members:
        half = width // 2
        pieces.append((distance, 0, lax.ppermute(forward[:, :half], axis_name, up)))
        pieces.append((distance, half, lax.ppermute(backward[:, half:], axis_name, down)))
    for offset, inner, piece in pieces:
        column = lax.rem(me + offset, members) * width + inner
        gathered = lax.dynamic_update_slice(gathered, piece, (0, column))
    return gathered


def project(rows, weight_blocks, member):
    depth = weight_blocks[0].shape[0]
    total = None
    for entry, block in enumerate(weight_blocks):
        columns = lax.dynamic_slice_in_dim(rows, (member ^ entry) * depth, depth, 1)
        share = jnp.dot(columns, block, preferred_element_type=jnp.float32)
        total = share if total is None else total + share
    return total


def per_device(
    patches,
    patch_counts,
    placement,
    positions,
    text_embeds,
    vit_gain,
    vit_qkv,
    vit_proj,
    merger_gain,
    merger_up,
    merger_down,
    llm_gain,
    llm_query,
    llm_key,
    llm_value,
):
    width_wide = lax.axis_size("wide")
    myself = lax.axis_index("wide")
    capacity = MAXM * ((IMG_DEV + width_wide - 1) // width_wide)
    local_heads = vit_qkv.shape[2] // VHD
    own_weights = jnp.concatenate([llm_query, llm_key, llm_value], axis=1)
    weight_blocks = doubling_gather(own_weights, "wide")
    members = lax.axis_size("tp")
    patch_rows = patches.astype(jnp.float32)
    normed = layer_norm(patch_rows, vit_gain).astype(jnp.bfloat16)
    triple = jnp.dot(normed, vit_qkv.reshape(VD, -1), preferred_element_type=jnp.float32).astype(
        jnp.bfloat16
    )
    triple = triple.reshape(IMG_DEV, MAXP, 3, local_heads, VHD)
    scores = jnp.einsum(
        "iqhd,ikhd->ihqk", triple[:, :, 0], triple[:, :, 1], preferred_element_type=jnp.float32
    ) * VHD ** (-0.5)
    own_counts = lax.dynamic_slice_in_dim(patch_counts, myself * IMG_DEV, IMG_DEV)
    present = jnp.arange(MAXP)[None, :] < own_counts[:, None]
    scores = jnp.where(present[:, None, None, :], scores, -jnp.inf)
    highest = jnp.max(scores, axis=-1, keepdims=True)
    raised = jnp.exp(scores - highest)
    attention_weights = (raised / jnp.sum(raised, axis=-1, keepdims=True)).astype(jnp.bfloat16)
    context = jnp.einsum(
        "ihqk,ikhd->iqhd", attention_weights, triple[:, :, 2], preferred_element_type=jnp.float32
    ).astype(jnp.bfloat16)
    context = context.reshape(IMG_DEV * MAXP, local_heads * VHD)
    partial_heads = jnp.dot(context, vit_proj, preferred_element_type=jnp.float32)
    attended = exchange_sum(partial_heads.astype(jnp.bfloat16), "tp", 0)
    own_rows = IMG_DEV * MAXP // members
    own_patches = lax.dynamic_slice_in_dim(patches, lax.axis_index("tp") * own_rows, own_rows, 0)
    mixed_rows = own_patches.astype(jnp.float32) + attended
    own_merged = layer_norm(mixed_rows, merger_gain).astype(jnp.bfloat16)
    own_merged = own_merged.reshape(own_rows * MAXM // MAXP, 4 * VD)
    merged_in = lax.all_gather(own_merged, "tp", axis=0, tiled=True)
    half_rows = TOK_DEV // 2
    early_text = lax.optimization_barrier((text_embeds[:half_rows], merged_in))[0]
    early_text = ring_gather_columns(early_text, "tp")
    hidden = jax.nn.gelu(
        jnp.dot(merged_in, merger_up, preferred_element_type=jnp.float32), approximate=False
    ).astype(jnp.bfloat16)
    partial_visual = jnp.dot(hidden, merger_down, preferred_element_type=jnp.float32)
    send_index, send_live, take_index, take_live = handoff_tables(
        patch_counts, placement, width_wide, myself, capacity
    )
    visual = exchange_sum(partial_visual.astype(jnp.bfloat16), "tp", 1).astype(jnp.bfloat16)
    late_text = lax.optimization_barrier((text_embeds[half_rows:], visual))[0]
    late_text = ring_gather_columns(late_text, "tp")
    outgoing = pack_rows(visual, send_index, send_live)
    incoming = lax.all_to_all(outgoing, "wide", split_axis=0, concat_axis=0, tiled=True)
    incoming = incoming.reshape(-1, incoming.shape[-1])
    copies = jnp.broadcast_to(incoming[None], (members,) + incoming.shape)
    spread_rows = lax.all_to_all(copies, "tp", split_axis=0, concat_axis=0, tiled=True)
    spread_rows = lax.optimization_barrier((spread_rows, weight_blocks[-2]))[0]
    visual_rows = jnp.swapaxes(spread_rows, 0, 1).reshape(incoming.shape[0], -1)
    tables = rotary_tables(positions)
    results = []
    for first_row, text_rows in ((0, early_text), (half_rows, late_text)):
        rows = slice(first_row, first_row + half_rows)
        prompt_rows = place_rows(visual_rows, take_index[rows], take_live[rows], text_rows)
        normed_prompt = rms_norm(prompt_rows.astype(jnp.float32), llm_gain).astype(jnp.bfloat16)
        projected = project(normed_prompt, weight_blocks, myself)
        first = llm_query.shape[1]
        second = first + llm_key.shape[1]
        turned = rotary(
            projected[:, :second].reshape(half_rows, -1, HD), (tables[0][rows], tables[1][rows])
        )
        turned = turned.astype(jnp.bfloat16).reshape(half_rows, -1)
        results.append((turned[:, :first], turned[:, first:], projected[:, second:].astype(jnp.bfloat16)))
    return tuple(jnp.concatenate(pair, axis=0) for pair in zip(*results))


def solution(mesh):
    return jax.shard_map(
        per_device,
        mesh=mesh,
        in_specs=(
            P(("groups", "wide"), None),
            P("groups"),
            P("groups", None),
            P(None, ("groups", "wide")),
            P(("groups", "wide"), "tp"),
            P(),
            P(None, None, "tp"),
            P("tp", None),
            P(),
            P(None, "tp"),
            P("tp", None),
            P(),
            P("wide", "tp"),
            P("wide", "tp"),
            P("wide", "tp"),
        ),
        out_specs=(
            P(("groups", "wide"), "tp"),
            P(("groups", "wide"), "tp"),
            P(("groups", "wide"), "tp"),
        ),
        check_vma=False,
    )
```

```python
import jax
import jax.numpy as jnp
from jax import lax
from jax.sharding import PartitionSpec as P

VD = 1280
HD = 128
IMG_DEV = 8
MAXP = 32
TOK_DEV = 512
VHD = 80
MAXM = 8


NORM_EPS = 1e-06
ROPE_BASE = 1000000.0


def layer_norm(inputs, scale_gain):
    center = jnp.mean(inputs, axis=-1, keepdims=True)
    shifted = inputs - center
    spread = jnp.mean(shifted * shifted, axis=-1, keepdims=True)
    return shifted * lax.rsqrt(spread + NORM_EPS) * scale_gain


def rms_norm(inputs, scale_gain):
    square = jnp.mean(inputs * inputs, axis=-1, keepdims=True)
    return inputs * lax.rsqrt(square + NORM_EPS) * scale_gain


def rotary(values, positions):
    half_size = HD // 2
    frequency = jnp.arange(half_size).astype(jnp.float32)
    inverse = ROPE_BASE ** (-2.0 * frequency / HD)
    first_end = HD // 8
    second = first_end + 3 * HD // 16
    ordinal = jnp.arange(half_size)
    section = jnp.where(ordinal < first_end, 0, jnp.where(ordinal < second, 1, 2))
    chosen = jnp.where(
        section[:, None] == 0,
        positions[0][None, :],
        jnp.where(section[:, None] == 1, positions[1][None, :], positions[2][None, :]),
    )
    angles = chosen.T.astype(jnp.float32) * inverse[None, :]
    angles = jnp.concatenate([angles, angles], axis=1)
    cosine = jnp.cos(angles)[:, None, :]
    sine_table = jnp.sin(angles)[:, None, :]
    upper_half = values[..., :half_size]
    lower_half = values[..., half_size:]
    turned = jnp.concatenate([-lower_half, upper_half], axis=-1)
    return values * cosine + turned * sine_table


def handoff_tables(patch_counts, placement, width_wide, myself, capacity):
    merged_count = patch_counts // 4
    owners = placement[:, 0]
    starts = placement[:, 1]
    owner_grid = owners.reshape(width_wide, IMG_DEV)
    count_grid = merged_count.reshape(width_wide, IMG_DEV)
    ordinal = jnp.arange(IMG_DEV)
    before = ordinal[:, None] < ordinal[None, :]
    same_owner = owner_grid[:, :, None] == owner_grid[:, None, :]
    offsets = jnp.sum(jnp.where(same_owner & before[None], count_grid[:, :, None], 0), axis=1)
    mine_owner = lax.dynamic_index_in_dim(owner_grid, myself, 0, keepdims=False)
    mine_count = lax.dynamic_index_in_dim(count_grid, myself, 0, keepdims=False)
    mine_offset = lax.dynamic_index_in_dim(offsets, myself, 0, keepdims=False)
    target = jnp.arange(width_wide)[:, None, None]
    slot_index = jnp.arange(capacity)[None, :, None]
    matches = (
        (mine_owner[None, None, :] == target)
        & (slot_index >= mine_offset[None, None, :])
        & (slot_index < mine_offset[None, None, :] + mine_count[None, None, :])
    )
    source_row = ordinal[None, None, :] * MAXM + slot_index - mine_offset[None, None, :]
    send_index = jnp.sum(jnp.where(matches, source_row, 0), axis=-1)
    send_live = jnp.any(matches, axis=-1)
    row_place = jnp.arange(TOK_DEV)[:, None]
    inside = (
        (owners[None, :] == myself)
        & (row_place >= starts[None, :])
        & (row_place < starts[None, :] + merged_count[None, :])
    )
    image_source = jnp.arange(owners.shape[0]) // IMG_DEV
    flat_slot = (
        image_source[None, :] * capacity
        + offsets.reshape(-1)[None, :]
        + row_place
        - starts[None, :]
    )
    take_index = jnp.sum(jnp.where(inside, flat_slot, 0), axis=-1)
    take_live = jnp.any(inside, axis=-1)
    return (send_index, send_live, take_index, take_live)


def pack_rows(visual, send_index, send_live):
    picked = jnp.take(visual, send_index.reshape(-1), axis=0)
    picked = picked.reshape(send_index.shape + (visual.shape[1],))
    return jnp.where(send_live[..., None], picked, jnp.zeros((), visual.dtype))


def exchange_sum(partial, axis_name, split_axis):
    members = lax.axis_size(axis_name)
    shape = partial.shape
    cut = shape[:split_axis] + (members, shape[split_axis] // members) + shape[split_axis + 1 :]
    stacked = jnp.moveaxis(partial.reshape(cut), split_axis, 0)
    swapped = lax.all_to_all(stacked, axis_name, split_axis=0, concat_axis=0, tiled=True)
    return jnp.sum(swapped.astype(jnp.float32), axis=0)


def doubling_gather(block, axis_name):
    members = lax.axis_size(axis_name)
    held = {0: block}
    bits = []
    step = 1
    while step < members:
        bits.append(step)
        step *= 2
    for bit in bits[1:] + bits[:1]:
        pairs = [(source, source ^ bit) for source in range(members)]
        for entry in sorted(held):
            held[entry ^ bit] = lax.ppermute(held[entry], axis_name, pairs)
    return [held[entry] for entry in range(members)]


def ring_gather_columns(block, axis_name):
    members = lax.axis_size(axis_name)
    me = lax.axis_index(axis_name)
    width = block.shape[1]
    up = [(source, (source + 1) % members) for source in range(members)]
    down = [(source, (source - 1) % members) for source in range(members)]
    gathered = jnp.zeros((block.shape[0], width * members), block.dtype)
    pieces = [(0, 0, block)]
    forward, backward = block, block
    distance = 1
    while 2 * distance < members:
        forward = lax.ppermute(forward, axis_name, up)
        backward = lax.ppermute(backward, axis_name, down)
        pieces.append((members - distance, 0, forward))
        pieces.append((distance, 0, backward))
        distance += 1
    if 2 * distance == members:
        half = width // 2
        pieces.append((distance, 0, lax.ppermute(forward[:, :half], axis_name, up)))
        pieces.append((distance, half, lax.ppermute(backward[:, half:], axis_name, down)))
    for offset, inner, piece in pieces:
        column = lax.rem(me + offset, members) * width + inner
        gathered = lax.dynamic_update_slice(gathered, piece, (0, column))
    return gathered, [piece for _, _, piece in pieces[1:3]]


def project(rows, weight_blocks, member):
    depth = weight_blocks[0].shape[0]
    total = None
    for entry, block in enumerate(weight_blocks):
        columns = lax.dynamic_slice_in_dim(rows, (member ^ entry) * depth, depth, 1)
        share = jnp.dot(columns, block, preferred_element_type=jnp.float32)
        total = share if total is None else total + share
    return total


def per_device(
    patches,
    patch_counts,
    placement,
    positions,
    text_embeds,
    vit_gain,
    vit_qkv,
    vit_proj,
    merger_gain,
    merger_up,
    merger_down,
    llm_gain,
    llm_query,
    llm_key,
    llm_value,
):
    width_wide = lax.axis_size("wide")
    myself = lax.axis_index("wide")
    capacity = MAXM * ((IMG_DEV + width_wide - 1) // width_wide)
    local_heads = vit_qkv.shape[2] // VHD
    own_weights = jnp.concatenate([llm_query, llm_key, llm_value], axis=1)
    weight_blocks = doubling_gather(own_weights, "wide")
    text_rows, first_arrivals = ring_gather_columns(text_embeds, "tp")
    members = lax.axis_size("tp")
    patch_rows = patches.astype(jnp.float32)
    normed = layer_norm(patch_rows, vit_gain).astype(jnp.bfloat16)
    triple = jnp.dot(normed, vit_qkv.reshape(VD, -1), preferred_element_type=jnp.float32).astype(
        jnp.bfloat16
    )
    triple = triple.reshape(IMG_DEV, MAXP, 3, local_heads, VHD)
    scores = jnp.einsum(
        "iqhd,ikhd->ihqk", triple[:, :, 0], triple[:, :, 1], preferred_element_type=jnp.float32
    ) * VHD ** (-0.5)
    own_counts = lax.dynamic_slice_in_dim(patch_counts, myself * IMG_DEV, IMG_DEV)
    present = jnp.arange(MAXP)[None, :] < own_counts[:, None]
    scores = jnp.where(present[:, None, None, :], scores, -jnp.inf)
    highest = jnp.max(scores, axis=-1, keepdims=True)
    raised = jnp.exp(scores - highest)
    attention_weights = (raised / jnp.sum(raised, axis=-1, keepdims=True)).astype(jnp.bfloat16)
    context = jnp.einsum(
        "ihqk,ikhd->iqhd", attention_weights, triple[:, :, 2], preferred_element_type=jnp.float32
    ).astype(jnp.bfloat16)
    context = context.reshape(IMG_DEV * MAXP, local_heads * VHD)
    partial_heads = jnp.dot(context, vit_proj, preferred_element_type=jnp.float32)
    attended = exchange_sum(partial_heads.astype(jnp.bfloat16), "tp", 0)
    attended = lax.optimization_barrier((attended, first_arrivals))[0]
    own_rows = IMG_DEV * MAXP // members
    own_patches = lax.dynamic_slice_in_dim(patches, lax.axis_index("tp") * own_rows, own_rows, 0)
    mixed_rows = own_patches.astype(jnp.float32) + attended
    own_merged = layer_norm(mixed_rows, merger_gain).astype(jnp.bfloat16)
    own_merged = own_merged.reshape(own_rows * MAXM // MAXP, 4 * VD)
    merged_in = lax.all_gather(own_merged, "tp", axis=0, tiled=True)
    merged_in = lax.optimization_barrier((merged_in, weight_blocks[-2]))[0]
    hidden = jax.nn.gelu(
        jnp.dot(merged_in, merger_up, preferred_element_type=jnp.float32), approximate=False
    ).astype(jnp.bfloat16)
    partial_visual = jnp.dot(hidden, merger_down, preferred_element_type=jnp.float32)
    send_index, send_live, take_index, take_live = handoff_tables(
        patch_counts, placement, width_wide, myself, capacity
    )
    visual = exchange_sum(partial_visual.astype(jnp.bfloat16), "tp", 1).astype(jnp.bfloat16)
    outgoing = pack_rows(visual, send_index, send_live)
    incoming = lax.all_to_all(outgoing, "wide", split_axis=0, concat_axis=0, tiled=True)
    incoming = incoming.reshape(-1, incoming.shape[-1])
    copies = jnp.broadcast_to(incoming[None], (members,) + incoming.shape)
    spread_rows = lax.all_to_all(copies, "tp", split_axis=0, concat_axis=0, tiled=True)
    normed_text = rms_norm(text_rows.astype(jnp.float32), llm_gain).astype(jnp.bfloat16)
    projected_text = project(normed_text, weight_blocks, myself)
    spread_rows, projected_text = lax.optimization_barrier((spread_rows, projected_text))
    visual_rows = jnp.swapaxes(spread_rows, 0, 1).reshape(incoming.shape[0], -1)
    normed_visual = rms_norm(visual_rows.astype(jnp.float32), llm_gain).astype(jnp.bfloat16)
    projected_visual = project(normed_visual, weight_blocks, myself)
    placed = jnp.take(projected_visual, take_index, axis=0)
    projected = jnp.where(take_live[:, None], placed, projected_text)
    first = llm_query.shape[1]
    second = first + llm_key.shape[1]
    projected_query = projected[:, :first]
    projected_key = projected[:, first:second]
    projected_value = projected[:, second:]
    queries = (
        rotary(projected_query.reshape(TOK_DEV, -1, HD), positions)
        .astype(jnp.bfloat16)
        .reshape(TOK_DEV, -1)
    )
    key_rows = (
        rotary(projected_key.reshape(TOK_DEV, -1, HD), positions)
        .astype(jnp.bfloat16)
        .reshape(TOK_DEV, -1)
    )
    value_rows = projected_value.astype(jnp.bfloat16)
    return (queries, key_rows, value_rows)


def solution(mesh):
    return jax.shard_map(
        per_device,
        mesh=mesh,
        in_specs=(
            P(("groups", "wide"), None),
            P("groups"),
            P("groups", None),
            P(None, ("groups", "wide")),
            P(("groups", "wide"), "tp"),
            P(),
            P(None, None, "tp"),
            P("tp", None),
            P(),
            P(None, "tp"),
            P("tp", None),
            P(),
            P("wide", "tp"),
            P("wide", "tp"),
            P("wide", "tp"),
        ),
        out_specs=(
            P(("groups", "wide"), "tp"),
            P(("groups", "wide"), "tp"),
            P(("groups", "wide"), "tp"),
        ),
        check_vma=False,
    )
```
